32 devices in a mesh: groups: 2 (over y), dp: 4 (over z), tensor: 4 (over x, core).
Axes of the slice: x: 2, y: 2, z: 4, core: 2. Of those that a mesh axis runs over, the one named last changes fastest.
Arguments:
- patches: bfloat16 [8192, 1280], P(('groups', 'dp')), parts along dimension 0, may hold values from -64 to 64
- grids: int32 [8, 2], P(('groups', 'dp')), parts along dimension 0, may hold values from 16 to 32, as said below
- dest: int32 [8, 256], P(('groups', 'dp')), parts along dimension 0, may hold values from 0 to 1535, as said below
- norm_gain: float32 [1280], replicated, may hold values from 0.1 to 1.9
- qkv_weight: bfloat16 [3, 1280, 1280], P(None, None, 'tensor'), may hold values from -8 to 8
- qkv_bias: float32 [3, 1280], P(None, 'tensor'), may hold values from -3 to 3
- proj_weight: bfloat16 [1280, 1280], P('tensor'), may hold values from -0.15625 to 0.15625
- proj_bias: float32 [1280], replicated, may hold values from -3 to 3
- merge_gain: float32 [1280], replicated, may hold values from 0.1 to 1.9
- w_first: bfloat16 [5120, 5120], P('dp', 'tensor'), may hold values from -0.078125 to 0.078125
- b_first: float32 [5120], P('tensor'), may hold values from -3 to 3
- w_second: bfloat16 [5120, 8192], P('tensor', 'dp'), may hold values from -0.078125 to 0.078125
- b_second: float32 [8192], P('tensor'), may hold values from -3 to 3
- text_embed: bfloat16 [3072, 8192], P(('groups', 'dp'), 'tensor'), parts along dimension 0, may hold values from -6 to 6
Outputs:
- sequence: bfloat16 [3072, 8192], P(('groups', 'dp'), 'tensor'), parts along dimension 0
The draws below stay inside these ranges and needn't reach their ends.
There are 2 independent parts, one for each index of `groups`. The reference program is written for one: setup_inputs(seed, part) draws one part's arguments, and reference() takes and returns one part's arrays. A program takes and returns all parts, laid end to end along the dimension named above; an argument that names none is the same for every part. Nothing has to cross between parts.
Inputs may be any that keep to these rules, and one draw needn't show every extreme that they name: `grids`: both sides of every grid are even, at least 16 and at most 32; in each part along `groups`, the first image (the one on dp index 0) has the full 32 x 32 grid. The rows dest[i, j] with j < grids[i, 0] * grids[i, 1] / 4 are distinct over all images; the live rows of one image reach at most 64 rows in each aligned block of 384 sequence rows, and exactly that many for a full grid.
All inputs are finite; a program needn't handle non-finite values.
Results may differ from the reference program's by a relative error of at most 0.014.
Values may be sent and summed in bfloat16 or wider, within the bound.
A program may use at most 128 MiB of HBM per device.

```python
import math
import jax
import jax.numpy as jnp
from jax import lax

V = 1280
HEADS = 16
HEAD_DIM = 80
D_LM = 8192
SIDE = 32
IMG_DEV = 1
IMAGES = 4
PATCHES = 1024
MERGED = 256
MERGE_W = 5120
ROWS = 4096
VIS = 1024
GAP = 128
SEQ_DP = 384
SEQ = 1536
BLOCK = 64
N_DP = 4
N_TENSOR = 4


def layout_helper(key):
    base = jax.random.fold_in(key, 4711)
    side_key, offset_key, order_key = jax.random.split(base, 3)
    halves = jax.random.randint(side_key, (IMAGES, 2), SIDE // 4, SIDE // 2 + 1)
    forced = jnp.arange(IMAGES)[:, None] < IMG_DEV
    halves = jnp.where(forced, SIDE // 2, halves)
    grid_sides = (2 * halves).astype(jnp.int32)
    offsets = jax.random.randint(offset_key, (IMAGES,), 0, GAP + 1)
    regions = jax.random.permutation(order_key, IMAGES)
    starts = regions * (MERGED + GAP) + offsets
    positions = starts[:, None] + jnp.arange(MERGED)[None, :]
    block_index = positions // BLOCK
    shard_index = block_index % N_DP
    local_row = block_index // N_DP * BLOCK + positions % BLOCK
    rows_out = (shard_index * SEQ_DP + local_row).astype(jnp.int32)
    return (grid_sides, rows_out)


def draw_grids(key, part):
    return layout_helper(key)[0]


def draw_dest(key, part):
    return layout_helper(key)[1]


def draw_patches(key, part):
    base_key = jax.random.fold_in(jax.random.fold_in(key, 31), 0)
    values = jax.random.normal(base_key, (ROWS, V), jnp.float32)
    return jnp.clip(values, -64.0, 64.0).astype(jnp.bfloat16)


def draw_qkv_weight(key, part):
    base_key = jax.random.fold_in(jax.random.fold_in(key, 57), 0)
    values = jax.random.normal(base_key, (3, V, V), jnp.float32) * V ** (-0.5)
    return jnp.clip(values, -8.0, 8.0).astype(jnp.bfloat16)


def levels(own_key, extent, pieces, low, top_value):
    def one(axis_at, parts):
        heights = jax.random.uniform(jax.random.fold_in(jax.random.fold_in(own_key, 6), axis_at), (parts,), jnp.float32, low / len(pieces), top_value / len(pieces))
        return jnp.repeat(jnp.exp(heights), extent[axis_at] // parts).reshape((-1,) + (1,) * (len(extent) - axis_at - 1))

    level = one(*pieces[0])
    for cut in pieces[1:]:
        level = level * one(*cut)
    return level


def centred(key, dims, spread, limit, shards=(), kind=jnp.bfloat16):
    result = spread * jax.random.normal(key, dims, jnp.float32)
    if shards:
        result = result * levels(key, dims, shards, -0.22, 0.18)
    return jnp.clip(result, -limit, limit).astype(kind)


def setup_inputs(seed: int = 0, part: int = 0) -> dict:
    key_list = jax.random.split(jax.random.key(seed), 15)
    part_splits = jax.random.split(jax.random.fold_in(key_list[14], part), 15)
    patches = draw_patches(jax.random.fold_in(jax.random.fold_in(key_list[14], part), 71), part)
    grids = draw_grids(jax.random.fold_in(jax.random.fold_in(key_list[14], part), 71), part)
    dest = draw_dest(jax.random.fold_in(jax.random.fold_in(key_list[14], part), 71), part)
    norm_gain = jnp.clip(1.0 + 0.18 * jax.random.normal(key_list[3], (V,), jnp.float32), 0.1, 1.9)
    qkv_weight = draw_qkv_weight(jax.random.fold_in(key_list[14], 71), part)
    qkv_bias = centred(key_list[5], (3, V), 0.5, 3.0, ((1, 4),), jnp.float32)
    proj_weight = centred(key_list[6], (V, V), V ** -0.5, 0.15625, ((0, 4),))
    proj_bias = centred(key_list[7], (V,), 0.5, 3.0, (), jnp.float32)
    merge_gain = jnp.clip(1.0 + 0.18 * jax.random.normal(key_list[8], (V,), jnp.float32), 0.1, 1.9)
    w_first = centred(key_list[9], (MERGE_W, MERGE_W), MERGE_W ** -0.5, 0.078125, ((0, 4), (1, 4)))
    b_first = centred(key_list[10], (MERGE_W,), 0.5, 3.0, ((0, 4),), jnp.float32)
    w_second = centred(key_list[11], (MERGE_W, D_LM), MERGE_W ** -0.5, 0.078125, ((0, 4), (1, 4)))
    b_second = centred(key_list[12], (D_LM,), 0.5, 3.0, ((0, 4),), jnp.float32)
    text_embed = centred(part_splits[13], (SEQ, D_LM), 1.0, 6.0, ((0, 4), (1, 4)))
    return dict(patches=patches, grids=grids, dest=dest, norm_gain=norm_gain, qkv_weight=qkv_weight, qkv_bias=qkv_bias, proj_weight=proj_weight, proj_bias=proj_bias, merge_gain=merge_gain, w_first=w_first, b_first=b_first, w_second=w_second, b_second=b_second, text_embed=text_embed)


def rms_scale(values, gain):
    return values * lax.rsqrt(lax.optimization_barrier(jnp.mean(values * values, axis=-1, keepdims=True)) + 1e-06) * gain

def reference(patches, grids, dest, norm_gain, qkv_weight, qkv_bias, proj_weight, proj_bias, merge_gain, w_first, b_first, w_second, b_second, text_embed):
    live_count = grids[:, 0] * grids[:, 1]
    image_rows = patches.reshape(IMAGES, PATCHES, V)

    def encode(image_item):
        rows_in, count_in = image_item
        normed = rms_scale(rows_in.astype(jnp.float32), norm_gain).astype(jnp.bfloat16)
        projected = jnp.einsum('rv,jvc->jrc', normed.astype(jnp.float32), qkv_weight.astype(jnp.float32)) + qkv_bias[:, None, :]
        projected = projected.astype(jnp.bfloat16).reshape(3, PATCHES, HEADS, HEAD_DIM)
        queries = projected[0].astype(jnp.float32)
        key_rows = projected[1].astype(jnp.float32)
        value_rows = projected[2].astype(jnp.float32)
        scores = jnp.einsum('qhd,khd->hqk', queries, key_rows) / math.sqrt(HEAD_DIM)
        live_keys = jnp.arange(PATCHES, dtype=jnp.int32) < count_in
        scores = jnp.where(live_keys[None, None, :], scores, jnp.float32(-1e+30))
        peak_score = lax.optimization_barrier(jnp.max(scores, axis=-1, keepdims=True))
        exponent = jnp.exp(scores - peak_score)
        weights = (exponent / lax.optimization_barrier(jnp.sum(exponent, axis=-1, keepdims=True))).astype(jnp.bfloat16)
        attended = jnp.einsum('hqk,khd->qhd', weights.astype(jnp.float32), value_rows)
        return attended.astype(jnp.bfloat16).reshape(PATCHES, V)
    attended = lax.map(encode, (image_rows, live_count)).reshape(ROWS, V)
    group_width = V // N_TENSOR
    summed = jnp.zeros((ROWS, V), jnp.float32)
    for group in range(N_TENSOR):
        part_rows = jnp.dot(attended[:, group * group_width:(group + 1) * group_width], proj_weight[group * group_width:(group + 1) * group_width], preferred_element_type=jnp.float32)
        summed = summed + part_rows.astype(jnp.bfloat16).astype(jnp.float32)
    resid = patches.astype(jnp.float32) + summed + proj_bias
    merged_in = rms_scale(resid, merge_gain).astype(jnp.bfloat16).reshape(VIS, MERGE_W)
    first_out = jnp.dot(merged_in, w_first, preferred_element_type=jnp.float32) + b_first
    hidden = jax.nn.gelu(first_out, approximate=False).astype(jnp.bfloat16)
    hidden_width = MERGE_W // N_TENSOR
    visual = jnp.zeros((VIS, D_LM), jnp.float32)
    for group in range(N_TENSOR):
        second_rows = jnp.dot(hidden[:, group * hidden_width:(group + 1) * hidden_width], w_second[group * hidden_width:(group + 1) * hidden_width], preferred_element_type=jnp.float32)
        visual = visual + second_rows.astype(jnp.bfloat16).astype(jnp.float32)
    visual = (visual + b_second).astype(jnp.bfloat16)
    live_rows = jnp.arange(MERGED, dtype=jnp.int32)[None, :] < (live_count // 4)[:, None]
    target = jnp.where(live_rows, dest, SEQ).astype(jnp.int32).reshape(VIS)
    sequence = text_embed.at[target].set(visual, mode='drop')
    return sequence
```

```python
import math

import jax
import jax.numpy as jnp
from jax import lax
from jax.sharding import PartitionSpec as P

HEAD_DIM = 80
PATCHES = 1024
MERGED = 256


def rms_scale(values, gain):
    return values * lax.rsqrt(jnp.mean(values * values, axis=-1, keepdims=True) + 1e-06) * gain


def placement(dest, live_count, dp_count, seq_rows, capacity):
    merged_dev = dest.size
    live_rows = (jnp.arange(MERGED, dtype=jnp.int32)[None, :] < (live_count // 4)[:, None]).reshape(merged_dev)
    dest_flat = dest.reshape(merged_dev)
    shard_id = jnp.where(live_rows, dest_flat // seq_rows, dp_count)
    local_row = dest_flat % seq_rows
    index = jnp.arange(merged_dev, dtype=jnp.int32)
    earlier = (shard_id[:, None] == shard_id[None, :]) & (index[None, :] < index[:, None])
    rank = jnp.sum(earlier.astype(jnp.int32), axis=1)
    slot = jnp.where(live_rows & (rank < capacity), shard_id * capacity + rank, -1)
    hit = jnp.arange(dp_count * capacity, dtype=jnp.int32)[:, None] == slot[None, :]
    rows = jnp.max(jnp.where(hit, local_row[None, :], -1), axis=1)
    return hit.astype(jnp.bfloat16), rows


def attention(patches, live_count, norm_gain, qkv_weight, qkv_bias, images_dev, heads_dev):
    normed = rms_scale(patches.astype(jnp.float32), norm_gain).astype(jnp.bfloat16)
    projected = (
        jnp.einsum("rv,jvc->jrc", normed, qkv_weight, preferred_element_type=jnp.float32)
        + qkv_bias[:, None, :]
    )
    projected = projected.astype(jnp.bfloat16).reshape(3, images_dev, PATCHES, heads_dev, HEAD_DIM)
    scores = jnp.einsum(
        "iqhd,ikhd->ihqk", projected[0], projected[1], preferred_element_type=jnp.float32
    ) / math.sqrt(HEAD_DIM)
    live_keys = jnp.arange(PATCHES, dtype=jnp.int32)[None, :] < live_count[:, None]
    scores = jnp.where(live_keys[:, None, None, :], scores, jnp.float32(-1e30))
    peak_score = jnp.max(scores, axis=-1, keepdims=True)
    exponent = jnp.exp(scores - peak_score)
    weights = (exponent / jnp.sum(exponent, axis=-1, keepdims=True)).astype(jnp.bfloat16)
    attended = jnp.einsum(
        "ihqk,ikhd->iqhd", weights, projected[2], preferred_element_type=jnp.float32
    )
    return attended.astype(jnp.bfloat16).reshape(patches.shape[0], heads_dev * HEAD_DIM)


def local(
    patches,
    grids,
    dest,
    norm_gain,
    qkv_weight,
    qkv_bias,
    proj_weight,
    proj_bias,
    merge_gain,
    w_first,
    b_first,
    w_second,
    b_second,
    text_embed,
):
    rows_dev, width = patches.shape
    images_dev = grids.shape[0]
    heads_dev = qkv_weight.shape[2] // HEAD_DIM
    dp_count = lax.axis_size("dp")
    tensor_count = lax.axis_size("tensor")
    seq_rows = text_embed.shape[0]
    capacity = images_dev * (MERGED // dp_count)
    live_count = grids[:, 0] * grids[:, 1]
    permute, slot_rows = placement(dest, live_count, dp_count, seq_rows, capacity)
    arrived_rows = lax.all_to_all(
        slot_rows.reshape(dp_count, capacity), "dp", split_axis=0, concat_axis=0, tiled=True
    ).reshape(-1)

    attended = attention(patches, live_count, norm_gain, qkv_weight, qkv_bias, images_dev, heads_dev)
    partial_value = jnp.dot(attended, proj_weight, preferred_element_type=jnp.float32).astype(jnp.bfloat16)
    summed = lax.psum_scatter(partial_value, "tensor", scatter_dimension=0, tiled=True).astype(jnp.float32)
    part = rows_dev // tensor_count
    own = lax.dynamic_slice_in_dim(patches, lax.axis_index("tensor") * part, part, 0)
    resid = own.astype(jnp.float32) + summed + proj_bias
    merged_in = rms_scale(resid, merge_gain).astype(jnp.bfloat16).reshape(part // 4, 4 * width)
    sliced = lax.all_to_all(
        merged_in.reshape(part // 4, dp_count, 4 * width // dp_count), "dp", split_axis=1, concat_axis=0, tiled=False
    )
    received = lax.all_gather(sliced, "tensor", axis=1, tiled=False)
    received = received.reshape(-1, 4 * width // dp_count)
    first_out = lax.psum_scatter(
        jnp.dot(received, w_first, preferred_element_type=jnp.float32).astype(jnp.bfloat16),
        "dp",
        scatter_dimension=0,
        tiled=True,
    ).astype(jnp.float32)
    hidden = jax.nn.gelu(first_out + b_first, approximate=False).astype(jnp.bfloat16)
    hidden = jnp.dot(permute, hidden, preferred_element_type=jnp.float32).astype(jnp.bfloat16)
    slots = lax.all_gather(hidden, "dp", axis=0, tiled=True)
    second = jnp.dot(slots, w_second, preferred_element_type=jnp.float32).astype(jnp.bfloat16)
    second = lax.psum_scatter(second, "tensor", scatter_dimension=1, tiled=True)
    columns = second.shape[1]
    second = second.reshape(dp_count, dp_count, capacity, columns)
    second = lax.all_to_all(second, "dp", split_axis=1, concat_axis=0, tiled=False)
    blocks = dp_count // tensor_count
    second = second.reshape(tensor_count, blocks, dp_count * capacity, columns)
    second = lax.all_to_all(second, "tensor", split_axis=0, concat_axis=0, tiled=True)
    visual = second.transpose(2, 1, 0, 3).reshape(dp_count * capacity, -1)
    visual = (visual.astype(jnp.float32) + b_second).astype(jnp.bfloat16)
    hit = jnp.arange(seq_rows, dtype=jnp.int32)[:, None] == arrived_rows[None, :]
    placed = jnp.dot(hit.astype(jnp.bfloat16), visual, preferred_element_type=jnp.float32).astype(jnp.bfloat16)
    return jnp.where(jnp.any(hit, axis=1)[:, None], placed, text_embed)


def solution(mesh):
    in_specs = (
        P(("groups", "dp"), None),
        P(("groups", "dp"), None),
        P(("groups", "dp"), None),
        P(),
        P(None, None, "tensor"),
        P(None, "tensor"),
        P("tensor", None),
        P(),
        P(),
        P("dp", "tensor"),
        P("tensor"),
        P("tensor", "dp"),
        P("tensor"),
        P(("groups", "dp"), "tensor"),
    )
    out_specs = P(("groups", "dp"), "tensor")
    return jax.shard_map(local, mesh=mesh, in_specs=in_specs, out_specs=out_specs, check_vma=False)
```

```python
import functools
import math

import jax
import jax.numpy as jnp
from jax import lax
from jax.experimental import pallas as pl
from jax.experimental.pallas import tpu as pltpu
from jax.sharding import PartitionSpec as P

MESH = pl.DeviceIdType.MESH

HEAD_DIM = 80
PATCHES = 1024
MERGED = 256


def rms_scale(values, gain):
    return values * lax.rsqrt(jnp.mean(values * values, axis=-1, keepdims=True) + 1e-06) * gain


def placement(dest, live_count, dp_count, seq_rows, capacity):
    merged_dev = dest.size
    live_rows = (jnp.arange(MERGED, dtype=jnp.int32)[None, :] < (live_count // 4)[:, None]).reshape(merged_dev)
    dest_flat = dest.reshape(merged_dev)
    shard_id = jnp.where(live_rows, dest_flat // seq_rows, dp_count)
    local_row = dest_flat % seq_rows
    index = jnp.arange(merged_dev, dtype=jnp.int32)
    earlier = (shard_id[:, None] == shard_id[None, :]) & (index[None, :] < index[:, None])
    rank = jnp.sum(earlier.astype(jnp.int32), axis=1)
    slot = jnp.where(live_rows & (rank < capacity), shard_id * capacity + rank, -1)
    hit = jnp.arange(dp_count * capacity, dtype=jnp.int32)[:, None] == slot[None, :]
    rows = jnp.max(jnp.where(hit, local_row[None, :], -1), axis=1)
    return hit.astype(jnp.bfloat16), rows


def attention(patches, live_count, norm_gain, qkv_weight, qkv_bias, images_dev, heads_dev):
    normed = rms_scale(patches.astype(jnp.float32), norm_gain).astype(jnp.bfloat16)
    projected = (
        jnp.einsum("rv,jvc->jrc", normed, qkv_weight, preferred_element_type=jnp.float32)
        + qkv_bias[:, None, :]
    )
    projected = projected.astype(jnp.bfloat16).reshape(3, images_dev, PATCHES, heads_dev, HEAD_DIM)
    scores = jnp.einsum(
        "iqhd,ikhd->ihqk", projected[0], projected[1], preferred_element_type=jnp.float32
    ) / math.sqrt(HEAD_DIM)
    live_keys = jnp.arange(PATCHES, dtype=jnp.int32)[None, :] < live_count[:, None]
    scores = jnp.where(live_keys[:, None, None, :], scores, jnp.float32(-1e30))
    peak_score = jnp.max(scores, axis=-1, keepdims=True)
    exponent = jnp.exp(scores - peak_score)
    weights = (exponent / jnp.sum(exponent, axis=-1, keepdims=True)).astype(jnp.bfloat16)
    attended = jnp.einsum(
        "ihqk,ikhd->iqhd", weights, projected[2], preferred_element_type=jnp.float32
    )
    return attended.astype(jnp.bfloat16).reshape(patches.shape[0], heads_dev * HEAD_DIM)


def merger_kernel(
    n, x_hbm, w1_hbm, bias, permute, w2_hbm, out_hbm,
    x, w1, w2, part, from_left, from_right, total, slots, acc, out,
    load_sem, sum_send, sum_recv, hid_send, hid_recv,
):
    chunks, _, block, wide = part.shape
    me = lax.axis_index("dp")
    left, right = lax.max(me - 1, 0), lax.min(me + 1, n - 1)
    has_left, has_right = me > 0, me < n - 1
    inner = has_left & has_right

    loads = [
        pltpu.make_async_copy(a, b, load_sem.at[i])
        for i, (a, b) in enumerate(((x_hbm, x), (w1_hbm, w1), (w2_hbm, w2)))
    ]
    for load in loads:
        load.start()

    barrier = pltpu.get_barrier_semaphore()

    @pl.when(has_left)
    def _():
        pl.semaphore_signal(barrier, inc=1, device_id={"dp": left}, device_id_type=MESH)

    @pl.when(has_right)
    def _():
        pl.semaphore_signal(barrier, inc=1, device_id={"dp": right}, device_id_type=MESH)

    pl.semaphore_wait(barrier, has_left.astype(jnp.int32) + has_right.astype(jnp.int32))

    def sum_right(c, b):
        return pltpu.make_async_remote_copy(
            part.at[c, b], from_left.at[c, b], sum_send.at[0, c, b], sum_recv.at[0, c, b],
            device_id={"dp": right}, device_id_type=MESH)

    def sum_left(c, b):
        return pltpu.make_async_remote_copy(
            part.at[c, b], from_right.at[c, b], sum_send.at[1, c, b], sum_recv.at[1, c, b],
            device_id={"dp": left}, device_id_type=MESH)

    def hid_right(c, b):
        return pltpu.make_async_remote_copy(
            slots.at[c, b], slots.at[c, b], hid_send.at[0, c, b], hid_recv.at[0, c, b],
            device_id={"dp": right}, device_id_type=MESH)

    def hid_left(c, b):
        return pltpu.make_async_remote_copy(
            slots.at[c, b], slots.at[c, b], hid_send.at[1, c, b], hid_recv.at[1, c, b],
            device_id={"dp": left}, device_id_type=MESH)

    def first(c):
        columns = pl.ds(pl.multiple_of(c * wide, wide), wide)

        def tile(b):
            part[c, b] = jnp.dot(
                x[pl.ds(pl.multiple_of(b * block, block), block), :], w1[:, columns],
                preferred_element_type=jnp.float32,
            ).astype(jnp.bfloat16)

        def up(i, carry):
            b = n - 1 - i
            tile(b)

            @pl.when((me == 0) & (b > 0))
            def _():
                sum_right(c, b).start()

            return carry

        def down(b, carry):
            tile(b)

            @pl.when((me == n - 1) & (b < n - 1))
            def _():
                sum_left(c, b).start()

            return carry

        @pl.when(me == 0)
        def _():
            lax.fori_loop(0, n, up, 0)

        @pl.when(me > 0)
        def _():
            lax.fori_loop(0, n, down, 0)

    def relay(c):
        def one(i, carry):
            b = n - 1 - i

            @pl.when(inner & (b > me))
            def _():
                sum_right(c, b).wait_recv()
                part[c, b] = (part[c, b].astype(jnp.float32) + from_left[c, b].astype(jnp.float32)).astype(jnp.bfloat16)
                sum_right(c, b).start()

            @pl.when(inner & (i < me))
            def _():
                sum_left(c, i).wait_recv()
                part[c, i] = (part[c, i].astype(jnp.float32) + from_right[c, i].astype(jnp.float32)).astype(jnp.bfloat16)
                sum_left(c, i).start()

            return carry

        lax.fori_loop(0, n, one, 0)

    def activate(c):
        total[...] = part[c, me].astype(jnp.float32) + bias[c]

        @pl.when(has_left)
        def _():
            sum_right(c, me).wait_recv()
            total[...] += from_left[c, me].astype(jnp.float32)

        @pl.when(has_right)
        def _():
            sum_left(c, me).wait_recv()
            total[...] += from_right[c, me].astype(jnp.float32)

        value = total[...]
        hidden = (0.5 * value * (1.0 + lax.erf(value * math.sqrt(0.5)))).astype(jnp.bfloat16)
        slots[c, me] = jnp.dot(permute[...], hidden, preferred_element_type=jnp.float32).astype(jnp.bfloat16)

        @pl.when(has_right)
        def _():
            hid_right(c, me).start()

        @pl.when(has_left)
        def _():
            hid_left(c, me).start()

    def spread(c):
        def one(k, carry):
            before, after = me - k, me + k

            @pl.when(before >= 0)
            def _():
                hid_right(c, before).wait_recv()

                @pl.when(has_right)
                def _():
                    hid_right(c, before).start()

            @pl.when(after < n)
            def _():
                hid_left(c, after).wait_recv()

                @pl.when(has_left)
                def _():
                    hid_left(c, after).start()

            return carry

        lax.fori_loop(1, n, one, 0)

    def second(c):
        depth = pl.ds(pl.multiple_of(c * wide, wide), wide)

        def one(b, carry):
            rows = pl.ds(pl.multiple_of(b * block, block), block)
            more = jnp.dot(slots[c, b], w2[depth, :], preferred_element_type=jnp.float32)

            @pl.when(c == 0)
            def _():
                acc[rows, :] = more

            @pl.when(c > 0)
            def _():
                acc[rows, :] += more

            return carry

        lax.fori_loop(0, n, one, 0)

    loads[0].wait()
    loads[1].wait()
    first(0)
    loads[2].wait()

    def step(s, carry):
        @pl.when(s + 1 < chunks)
        def _():
            first(s + 1)

        @pl.when(s < chunks)
        def _():
            relay(s)

        @pl.when((s >= 1) & (s <= chunks))
        def _():
            activate(s - 1)

        @pl.when(s >= 2)
        def _():
            spread(s - 2)
            second(s - 2)

        return carry

    lax.fori_loop(0, chunks + 2, step, 0)

    def finish(b, carry):
        rows = pl.ds(pl.multiple_of(b * block, block), block)
        out[rows, :] = acc[rows, :].astype(jnp.bfloat16)
        return carry

    lax.fori_loop(0, n, finish, 0)
    store = pltpu.make_async_copy(out, out_hbm, load_sem.at[0])
    store.start()

    def drain(c, carry):
        def one(b, inside):
            @pl.when(has_right & (b > me))
            def _():
                sum_right(c, b).wait_send()

            @pl.when(has_left & (b < me))
            def _():
                sum_left(c, b).wait_send()

            @pl.when(has_right & (b <= me))
            def _():
                hid_right(c, b).wait_send()

            @pl.when(has_left & (b >= me))
            def _():
                hid_left(c, b).wait_send()

            return inside

        return lax.fori_loop(0, n, one, carry)

    lax.fori_loop(0, chunks, drain, 0)
    store.wait()


def merger(x, w1, bias, permute, w2):
    n = lax.axis_size("dp")
    rows, depth = x.shape
    hidden, columns = w2.shape
    block = rows // n
    wide = 256 if hidden % 256 == 0 else 128
    chunks = hidden // wide
    any_space = pl.BlockSpec(memory_space=pl.ANY)
    vmem = pl.BlockSpec(memory_space=pltpu.VMEM)
    stack = pltpu.VMEM((chunks, n, block, wide), jnp.bfloat16)
    return pl.pallas_call(
        functools.partial(merger_kernel, n),
        out_shape=jax.ShapeDtypeStruct((rows, columns), jnp.bfloat16),
        in_specs=[any_space, any_space, vmem, vmem, any_space],
        out_specs=any_space,
        scratch_shapes=[
            pltpu.VMEM((rows, depth), jnp.bfloat16),
            pltpu.VMEM((depth, hidden), jnp.bfloat16),
            pltpu.VMEM((hidden, columns), jnp.bfloat16),
            stack,
            stack,
            stack,
            pltpu.VMEM((block, wide), jnp.float32),
            stack,
            pltpu.VMEM((rows, columns), jnp.float32),
            pltpu.VMEM((rows, columns), jnp.bfloat16),
            pltpu.SemaphoreType.DMA((3,)),
            pltpu.SemaphoreType.DMA((2, chunks, n)),
            pltpu.SemaphoreType.DMA((2, chunks, n)),
            pltpu.SemaphoreType.DMA((2, chunks, n)),
            pltpu.SemaphoreType.DMA((2, chunks, n)),
        ],
        compiler_params=pltpu.CompilerParams(
            collective_id=0, has_side_effects=True, vmem_limit_bytes=60 * 1024 * 1024
        ),
    )(x, w1, bias.reshape(chunks, 1, wide), permute, w2)


def local(
    patches,
    grids,
    dest,
    norm_gain,
    qkv_weight,
    qkv_bias,
    proj_weight,
    proj_bias,
    merge_gain,
    w_first,
    b_first,
    w_second,
    b_second,
    text_embed,
):
    rows_dev, width = patches.shape
    images_dev = grids.shape[0]
    heads_dev = qkv_weight.shape[2] // HEAD_DIM
    dp_count = lax.axis_size("dp")
    tensor_count = lax.axis_size("tensor")
    seq_rows = text_embed.shape[0]
    capacity = images_dev * (MERGED // dp_count)
    live_count = grids[:, 0] * grids[:, 1]
    permute, slot_rows = placement(dest, live_count, dp_count, seq_rows, capacity)
    arrived_rows = lax.all_to_all(
        slot_rows.reshape(dp_count, capacity), "dp", split_axis=0, concat_axis=0, tiled=True
    ).reshape(-1)

    attended = attention(patches, live_count, norm_gain, qkv_weight, qkv_bias, images_dev, heads_dev)
    partial_value = jnp.dot(attended, proj_weight, preferred_element_type=jnp.float32).astype(jnp.bfloat16)
    summed = lax.psum_scatter(partial_value, "tensor", scatter_dimension=0, tiled=True).astype(jnp.float32)
    part = rows_dev // tensor_count
    own = lax.dynamic_slice_in_dim(patches, lax.axis_index("tensor") * part, part, 0)
    resid = own.astype(jnp.float32) + summed + proj_bias
    merged_in = rms_scale(resid, merge_gain).astype(jnp.bfloat16).reshape(part // 4, 4 * width)
    sliced = lax.all_to_all(
        merged_in.reshape(part // 4, dp_count, 4 * width // dp_count), "dp", split_axis=1, concat_axis=0, tiled=False
    )
    received = lax.all_gather(sliced, "tensor", axis=1, tiled=False)
    received = received.reshape(-1, 4 * width // dp_count)
    second = merger(received, w_first, b_first, permute, w_second)
    second = lax.psum_scatter(second, "tensor", scatter_dimension=1, tiled=True)
    columns = second.shape[1]
    second = second.reshape(dp_count, dp_count, capacity, columns)
    second = lax.all_to_all(second, "dp", split_axis=1, concat_axis=0, tiled=False)
    blocks = dp_count // tensor_count
    second = second.reshape(tensor_count, blocks, dp_count * capacity, columns)
    second = lax.all_to_all(second, "tensor", split_axis=0, concat_axis=0, tiled=True)
    visual = second.transpose(2, 1, 0, 3).reshape(dp_count * capacity, -1)
    visual = (visual.astype(jnp.float32) + b_second).astype(jnp.bfloat16)
    hit = jnp.arange(seq_rows, dtype=jnp.int32)[:, None] == arrived_rows[None, :]
    placed = jnp.dot(hit.astype(jnp.bfloat16), visual, preferred_element_type=jnp.float32).astype(jnp.bfloat16)
    return jnp.where(jnp.any(hit, axis=1)[:, None], placed, text_embed)


def solution(mesh):
    in_specs = (
        P(("groups", "dp"), None),
        P(("groups", "dp"), None),
        P(("groups", "dp"), None),
        P(),
        P(None, None, "tensor"),
        P(None, "tensor"),
        P("tensor", None),
        P(),
        P(),
        P("dp", "tensor"),
        P("tensor"),
        P("tensor", "dp"),
        P("tensor"),
        P(("groups", "dp"), "tensor"),
    )
    out_specs = P(("groups", "dp"), "tensor")
    return jax.shard_map(local, mesh=mesh, in_specs=in_specs, out_specs=out_specs, check_vma=False)
```

```python
import functools
import math

import jax
import jax.numpy as jnp
from jax import lax
from jax.experimental import pallas as pl
from jax.experimental.pallas import tpu as pltpu
from jax.sharding import PartitionSpec as P

MESH = pl.DeviceIdType.MESH

HEAD_DIM = 80
PATCHES = 1024
MERGED = 256


def rms_scale(values, gain):
    return values * lax.rsqrt(jnp.mean(values * values, axis=-1, keepdims=True) + 1e-06) * gain


def placement(dest, live_count, dp_count, seq_rows, capacity):
    merged_dev = dest.size
    live_rows = (jnp.arange(MERGED, dtype=jnp.int32)[None, :] < (live_count // 4)[:, None]).reshape(merged_dev)
    dest_flat = dest.reshape(merged_dev)
    shard_id = jnp.where(live_rows, dest_flat // seq_rows, dp_count)
    local_row = dest_flat % seq_rows
    index = jnp.arange(merged_dev, dtype=jnp.int32)
    earlier = (shard_id[:, None] == shard_id[None, :]) & (index[None, :] < index[:, None])
    rank = jnp.sum(earlier.astype(jnp.int32), axis=1)
    slot = jnp.where(live_rows & (rank < capacity), shard_id * capacity + rank, -1)
    hit = jnp.arange(dp_count * capacity, dtype=jnp.int32)[:, None] == slot[None, :]
    rows = jnp.max(jnp.where(hit, local_row[None, :], -1), axis=1)
    return hit.astype(jnp.bfloat16), rows


def attention(patches, live_count, norm_gain, qkv_weight, qkv_bias, images_dev, heads_dev):
    normed = rms_scale(patches.astype(jnp.float32), norm_gain).astype(jnp.bfloat16)
    projected = (
        jnp.einsum("rv,jvc->jrc", normed, qkv_weight, preferred_element_type=jnp.float32)
        + qkv_bias[:, None, :]
    )
    projected = projected.astype(jnp.bfloat16).reshape(3, images_dev, PATCHES, heads_dev, HEAD_DIM)
    scores = jnp.einsum(
        "iqhd,ikhd->ihqk", projected[0], projected[1], preferred_element_type=jnp.float32
    ) / math.sqrt(HEAD_DIM)
    live_keys = jnp.arange(PATCHES, dtype=jnp.int32)[None, :] < live_count[:, None]
    scores = jnp.where(live_keys[:, None, None, :], scores, jnp.float32(-1e30))
    peak_score = jnp.max(scores, axis=-1, keepdims=True)
    exponent = jnp.exp(scores - peak_score)
    weights = (exponent / jnp.sum(exponent, axis=-1, keepdims=True)).astype(jnp.bfloat16)
    attended = jnp.einsum(
        "ihqk,ikhd->iqhd", weights, projected[2], preferred_element_type=jnp.float32
    )
    return attended.astype(jnp.bfloat16).reshape(patches.shape[0], heads_dev * HEAD_DIM)


def merger_kernel(
    n, x_hbm, w1_hbm, bias, permute, w2_hbm, out_hbm,
    x, w1, w2, part, from_left, from_right, total, slots, acc, out,
    load_sem, sum_send, sum_recv, hid_send, hid_recv,
):
    chunks, _, block, wide = part.shape
    me = lax.axis_index("dp")
    left, right = lax.max(me - 1, 0), lax.min(me + 1, n - 1)
    has_left, has_right = me > 0, me < n - 1
    inner = has_left & has_right

    loads = [
        pltpu.make_async_copy(a, b, load_sem.at[i])
        for i, (a, b) in enumerate(((x_hbm, x), (w1_hbm, w1), (w2_hbm, w2)))
    ]
    for load in loads:
        load.start()

    barrier = pltpu.get_barrier_semaphore()

    @pl.when(has_left)
    def _():
        pl.semaphore_signal(barrier, inc=1, device_id={"dp": left}, device_id_type=MESH)

    @pl.when(has_right)
    def _():
        pl.semaphore_signal(barrier, inc=1, device_id={"dp": right}, device_id_type=MESH)

    pl.semaphore_wait(barrier, has_left.astype(jnp.int32) + has_right.astype(jnp.int32))

    def sum_right(c, b):
        return pltpu.make_async_remote_copy(
            part.at[c, b], from_left.at[c, b], sum_send.at[0, c, b], sum_recv.at[0, c, b],
            device_id={"dp": right}, device_id_type=MESH)

    def sum_left(c, b):
        return pltpu.make_async_remote_copy(
            part.at[c, b], from_right.at[c, b], sum_send.at[1, c, b], sum_recv.at[1, c, b],
            device_id={"dp": left}, device_id_type=MESH)

    def hid_right(c, b):
        return pltpu.make_async_remote_copy(
            slots.at[c, b], slots.at[c, b], hid_send.at[0, c, b], hid_recv.at[0, c, b],
            device_id={"dp": right}, device_id_type=MESH)

    def hid_left(c, b):
        return pltpu.make_async_remote_copy(
            slots.at[c, b], slots.at[c, b], hid_send.at[1, c, b], hid_recv.at[1, c, b],
            device_id={"dp": left}, device_id_type=MESH)

    def first(c):
        columns = pl.ds(pl.multiple_of(c * wide, wide), wide)

        def tile(b):
            part[c, b] = jnp.dot(
                x[pl.ds(pl.multiple_of(b * block, block), block), :], w1[:, columns],
                preferred_element_type=jnp.float32,
            ).astype(jnp.bfloat16)

        def up(i, carry):
            b = n - 1 - i
            tile(b)

            @pl.when((me == 0) & (b > 0))
            def _():
                sum_right(c, b).start()

            return carry

        def down(b, carry):
            tile(b)

            @pl.when((me == n - 1) & (b < n - 1))
            def _():
                sum_left(c, b).start()

            return carry

        @pl.when(me == 0)
        def _():
            lax.fori_loop(0, n, up, 0)

        @pl.when(me > 0)
        def _():
            lax.fori_loop(0, n, down, 0)

    def relay(c):
        def one(i, carry):
            b = n - 1 - i

            @pl.when(inner & (b > me))
            def _():
                sum_right(c, b).wait_recv()
                part[c, b] = (part[c, b].astype(jnp.float32) + from_left[c, b].astype(jnp.float32)).astype(jnp.bfloat16)
                sum_right(c, b).start()

            @pl.when(inner & (i < me))
            def _():
                sum_left(c, i).wait_recv()
                part[c, i] = (part[c, i].astype(jnp.float32) + from_right[c, i].astype(jnp.float32)).astype(jnp.bfloat16)
                sum_left(c, i).start()

            return carry

        lax.fori_loop(0, n, one, 0)

    def activate(c):
        total[...] = part[c, me].astype(jnp.float32) + bias[c]

        @pl.when(has_left)
        def _():
            sum_right(c, me).wait_recv()
            total[...] += from_left[c, me].astype(jnp.float32)

        @pl.when(has_right)
        def _():
            sum_left(c, me).wait_recv()
            total[...] += from_right[c, me].astype(jnp.float32)

        value = total[...]
        hidden = (0.5 * value * (1.0 + lax.erf(value * math.sqrt(0.5)))).astype(jnp.bfloat16)
        slots[c, me] = jnp.dot(permute[...], hidden, preferred_element_type=jnp.float32).astype(jnp.bfloat16)

        @pl.when(has_right)
        def _():
            hid_right(c, me).start()

        @pl.when(has_left)
        def _():
            hid_left(c, me).start()

    def spread(c):
        def one(k, carry):
            before, after = me - k, me + k

            @pl.when(before >= 0)
            def _():
                hid_right(c, before).wait_recv()

                @pl.when(has_right)
                def _():
                    hid_right(c, before).start()

            @pl.when(after < n)
            def _():
                hid_left(c, after).wait_recv()

                @pl.when(has_left)
                def _():
                    hid_left(c, after).start()

            return carry

        lax.fori_loop(1, n, one, 0)

    def second(c):
        depth = pl.ds(pl.multiple_of(c * wide, wide), wide)

        def one(b, carry):
            rows = pl.ds(pl.multiple_of(b * block, block), block)
            more = jnp.dot(slots[c, b], w2[depth, :], preferred_element_type=jnp.float32)

            @pl.when(c == 0)
            def _():
                acc[rows, :] = more

            @pl.when(c > 0)
            def _():
                acc[rows, :] += more

            return carry

        lax.fori_loop(0, n, one, 0)

    loads[0].wait()
    loads[1].wait()
    first(0)
    loads[2].wait()

    def step(s, carry):
        @pl.when(s + 1 < chunks)
        def _():
            first(s + 1)

        @pl.when(s < chunks)
        def _():
            relay(s)

        @pl.when((s >= 1) & (s <= chunks))
        def _():
            activate(s - 1)

        @pl.when(s >= 2)
        def _():
            spread(s - 2)
            second(s - 2)

        return carry

    lax.fori_loop(0, chunks + 2, step, 0)

    def finish(b, carry):
        rows = pl.ds(pl.multiple_of(b * block, block), block)
        out[rows, :] = acc[rows, :].astype(jnp.bfloat16)
        return carry

    lax.fori_loop(0, n, finish, 0)
    store = pltpu.make_async_copy(out, out_hbm, load_sem.at[0])
    store.start()

    def drain(c, carry):
        def one(b, inside):
            @pl.when(has_right & (b > me))
            def _():
                sum_right(c, b).wait_send()

            @pl.when(has_left & (b < me))
            def _():
                sum_left(c, b).wait_send()

            @pl.when(has_right & (b <= me))
            def _():
                hid_right(c, b).wait_send()

            @pl.when(has_left & (b >= me))
            def _():
                hid_left(c, b).wait_send()

            return inside

        return lax.fori_loop(0, n, one, carry)

    lax.fori_loop(0, chunks, drain, 0)
    store.wait()


def merger(x, w1, bias, permute, w2):
    n = lax.axis_size("dp")
    rows, depth = x.shape
    hidden, columns = w2.shape
    block = rows // n
    wide = 256 if hidden % 256 == 0 else 128
    chunks = hidden // wide
    any_space = pl.BlockSpec(memory_space=pl.ANY)
    vmem = pl.BlockSpec(memory_space=pltpu.VMEM)
    stack = pltpu.VMEM((chunks, n, block, wide), jnp.bfloat16)
    return pl.pallas_call(
        functools.partial(merger_kernel, n),
        out_shape=jax.ShapeDtypeStruct((rows, columns), jnp.bfloat16),
        in_specs=[any_space, any_space, vmem, vmem, any_space],
        out_specs=any_space,
        scratch_shapes=[
            pltpu.VMEM((rows, depth), jnp.bfloat16),
            pltpu.VMEM((depth, hidden), jnp.bfloat16),
            pltpu.VMEM((hidden, columns), jnp.bfloat16),
            stack,
            stack,
            stack,
            pltpu.VMEM((block, wide), jnp.float32),
            stack,
            pltpu.VMEM((rows, columns), jnp.float32),
            pltpu.VMEM((rows, columns), jnp.bfloat16),
            pltpu.SemaphoreType.DMA((3,)),
            pltpu.SemaphoreType.DMA((2, chunks, n)),
            pltpu.SemaphoreType.DMA((2, chunks, n)),
            pltpu.SemaphoreType.DMA((2, chunks, n)),
            pltpu.SemaphoreType.DMA((2, chunks, n)),
        ],
        compiler_params=pltpu.CompilerParams(
            collective_id=0, has_side_effects=True, vmem_limit_bytes=60 * 1024 * 1024
        ),
    )(x, w1, bias.reshape(chunks, 1, wide), permute, w2)


def place_kernel(
    n, y, out, half, across_sum, from_across, ready, landed, got,
    mate_send, mate_recv, across_send, across_recv, row_send, row_recv, end_send, end_recv,
):
    quarter = y.shape[3] // 4
    row, me = lax.axis_index("dp"), lax.axis_index("tensor")
    core, side = me % 2, me // 2
    mate, across = side * 2 + 1 - core, (1 - side) * 2 + core

    barrier = pltpu.get_barrier_semaphore()
    for k in range(1, 4):
        pl.semaphore_signal(barrier, inc=1, device_id={"tensor": (me + k) % 4}, device_id_type=MESH)
    for k in range(1, n):
        pl.semaphore_signal(barrier, inc=1, device_id={"dp": (row + k) % n}, device_id_type=MESH)
    pl.semaphore_wait(barrier, 3 + n - 1)

    def piece(index):
        return pl.ds(pl.multiple_of(index * quarter, quarter), quarter)

    def to_mate(i, j):
        return pltpu.make_async_remote_copy(
            y.at[i, :, :, piece((side + j) % 2 * 2 + 1 - core)], half.at[i, j], mate_send.at[i, j], mate_recv.at[i, j],
            device_id={"tensor": mate}, device_id_type=MESH)

    def to_across(i):
        return pltpu.make_async_remote_copy(
            across_sum.at[i], from_across.at[i], across_send.at[i], across_recv.at[i],
            device_id={"tensor": across}, device_id_type=MESH)

    def to_row(i, k):
        other = (row + k) % n
        return pltpu.make_async_remote_copy(
            ready.at[i, other], landed.at[row, i], row_send.at[i, k], row_recv.at[i, k],
            device_id={"dp": other}, device_id_type=MESH)

    def to_end(i, k, block):
        return pltpu.make_async_remote_copy(
            landed.at[block, i], got.at[me, i], end_send.at[i, k], end_recv.at[i, me],
            device_id={"tensor": block}, device_id_type=MESH)

    for i in range(n):
        for j in (1, 0):
            to_mate(i, j).start()

    for i in range(n):
        to_mate(i, 1).wait_recv()
        for s in range(n):
            across_sum[i, s] = (
                y[i, s, :, piece((1 - side) * 2 + core)].astype(jnp.float32) + half[i, 1, s].astype(jnp.float32)
            ).astype(jnp.bfloat16)
        to_across(i).start()

    for i in range(n):
        to_mate(i, 0).wait_recv()
        to_across(i).wait_recv()
        for s in range(n):
            ready[i, s] = (
                y[i, s, :, piece(me)].astype(jnp.float32)
                + half[i, 0, s].astype(jnp.float32)
                + from_across[i, s].astype(jnp.float32)
            ).astype(jnp.bfloat16)
        for k in range(1, n):
            to_row(i, k).start()
        landed[row, i] = ready[i, row]

    for i in range(n):
        for k in range(n):
            block = (row + n - k) % n
            if k:
                to_row(i, k).wait_recv()

            @pl.when(block == me)
            def _():
                got[me, i] = landed[block, i]

            @pl.when(block != me)
            def _():
                to_end(i, k, block).start()

    for i in range(n):
        for k in range(1, 4):
            other = (me + k) % 4
            pltpu.make_async_remote_copy(
                landed.at[0, i], got.at[other, i], end_send.at[i, 0], end_recv.at[i, other],
                device_id={"tensor": other}, device_id_type=MESH).wait_recv()
    for t in range(4):
        out[:, :, t * quarter:(t + 1) * quarter] = got[t]

    for i in range(n):
        for j in range(2):
            to_mate(i, j).wait_send()
        to_across(i).wait_send()
        for k in range(1, n):
            to_row(i, k).wait_send()
        for k in range(n):
            block = (row + n - k) % n

            @pl.when(block != me)
            def _():
                to_end(i, k, block).wait_send()


def place(second):
    n, _, capacity, columns = second.shape
    quarter = columns // 4
    vmem = pl.BlockSpec(memory_space=pltpu.VMEM)
    stack = pltpu.VMEM((n, n, capacity, quarter), jnp.bfloat16)
    return pl.pallas_call(
        functools.partial(place_kernel, n),
        out_shape=jax.ShapeDtypeStruct((n, capacity, columns), jnp.bfloat16),
        in_specs=[vmem],
        out_specs=vmem,
        scratch_shapes=[
            pltpu.VMEM((n, 2, n, capacity, quarter), jnp.bfloat16),
            stack,
            stack,
            stack,
            stack,
            stack,
            pltpu.SemaphoreType.DMA((n, 2)),
            pltpu.SemaphoreType.DMA((n, 2)),
            pltpu.SemaphoreType.DMA((n,)),
            pltpu.SemaphoreType.DMA((n,)),
            pltpu.SemaphoreType.DMA((n, n)),
            pltpu.SemaphoreType.DMA((n, n)),
            pltpu.SemaphoreType.DMA((n, n)),
            pltpu.SemaphoreType.DMA((n, n)),
        ],
        compiler_params=pltpu.CompilerParams(
            collective_id=1, has_side_effects=True, vmem_limit_bytes=40 * 1024 * 1024
        ),
    )(second)


def exchange(second, dp_count, tensor_count, capacity):
    if dp_count == tensor_count == 4 and capacity % 16 == 0 and second.shape[1] % 512 == 0:
        return place(second.reshape(dp_count, dp_count, capacity, -1)).reshape(dp_count * capacity, -1)
    second = lax.psum_scatter(second, "tensor", scatter_dimension=1, tiled=True)
    columns = second.shape[1]
    second = second.reshape(dp_count, dp_count, capacity, columns)
    second = lax.all_to_all(second, "dp", split_axis=1, concat_axis=0, tiled=False)
    blocks = dp_count // tensor_count
    second = second.reshape(tensor_count, blocks, dp_count * capacity, columns)
    second = lax.all_to_all(second, "tensor", split_axis=0, concat_axis=0, tiled=True)
    return second.transpose(2, 1, 0, 3).reshape(dp_count * capacity, -1)


def local(
    patches,
    grids,
    dest,
    norm_gain,
    qkv_weight,
    qkv_bias,
    proj_weight,
    proj_bias,
    merge_gain,
    w_first,
    b_first,
    w_second,
    b_second,
    text_embed,
):
    rows_dev, width = patches.shape
    images_dev = grids.shape[0]
    heads_dev = qkv_weight.shape[2] // HEAD_DIM
    dp_count = lax.axis_size("dp")
    tensor_count = lax.axis_size("tensor")
    seq_rows = text_embed.shape[0]
    capacity = images_dev * (MERGED // dp_count)
    live_count = grids[:, 0] * grids[:, 1]
    permute, slot_rows = placement(dest, live_count, dp_count, seq_rows, capacity)
    arrived_rows = lax.all_to_all(
        slot_rows.reshape(dp_count, capacity), "dp", split_axis=0, concat_axis=0, tiled=True
    ).reshape(-1)

    attended = attention(patches, live_count, norm_gain, qkv_weight, qkv_bias, images_dev, heads_dev)
    partial_value = jnp.dot(attended, proj_weight, preferred_element_type=jnp.float32).astype(jnp.bfloat16)
    summed = lax.psum_scatter(partial_value, "tensor", scatter_dimension=0, tiled=True).astype(jnp.float32)
    part = rows_dev // tensor_count
    own = lax.dynamic_slice_in_dim(patches, lax.axis_index("tensor") * part, part, 0)
    resid = own.astype(jnp.float32) + summed + proj_bias
    merged_in = rms_scale(resid, merge_gain).astype(jnp.bfloat16).reshape(part // 4, 4 * width)
    sliced = lax.all_to_all(
        merged_in.reshape(part // 4, dp_count, 4 * width // dp_count), "dp", split_axis=1, concat_axis=0, tiled=False
    )
    received = lax.all_gather(sliced, "tensor", axis=1, tiled=False)
    received = received.reshape(-1, 4 * width // dp_count)
    second = merger(received, w_first, b_first, permute, w_second)
    visual = exchange(second, dp_count, tensor_count, capacity)
    visual = (visual.astype(jnp.float32) + b_second).astype(jnp.bfloat16)
    hit = jnp.arange(seq_rows, dtype=jnp.int32)[:, None] == arrived_rows[None, :]
    placed = jnp.dot(hit.astype(jnp.bfloat16), visual, preferred_element_type=jnp.float32).astype(jnp.bfloat16)
    return jnp.where(jnp.any(hit, axis=1)[:, None], placed, text_embed)


def solution(mesh):
    in_specs = (
        P(("groups", "dp"), None),
        P(("groups", "dp"), None),
        P(("groups", "dp"), None),
        P(),
        P(None, None, "tensor"),
        P(None, "tensor"),
        P("tensor", None),
        P(),
        P(),
        P("dp", "tensor"),
        P("tensor"),
        P("tensor", "dp"),
        P("tensor"),
        P(("groups", "dp"), "tensor"),
    )
    out_specs = P(("groups", "dp"), "tensor")
    return jax.shard_map(local, mesh=mesh, in_specs=in_specs, out_specs=out_specs, check_vma=False)
```
